512 devices in a mesh: group: 2 (over y), seq: 128 (over z, x), tensor: 2 (over core).
Axes of the slice: x: 4, y: 2, z: 32, core: 2. Of those that a mesh axis runs over, the one named last changes fastest.
The devices are a block of a 4x8x32 slice.
Arguments:
- queries: bfloat16 [64, 64, 128], P('group', 'tensor'), parts along dimension 0, may hold values from -10 to 10
- k_cache: bfloat16 [2048, 8, 128, 128], P(('group', 'seq'), 'tensor'), parts along dimension 0, may hold values from -6 to 6
- value_cache: bfloat16 [2048, 8, 128, 128], P(('group', 'seq'), 'tensor'), parts along dimension 0, may hold values from -6 to 6
- kv_lengths: int32 [64], P('group'), parts along dimension 0, may hold values from 1 to 32768, as said below
- page_table: int32 [64, 256], P('group'), parts along dimension 0, may hold values from -1 to 1023, as said below
- request_batch_row: int32 [64], P('group'), parts along dimension 0, may hold values from 0 to 31, each once
Outputs:
- attended: bfloat16 [64, 64, 128], P('group', 'tensor'), parts along dimension 0
The draws below stay inside these ranges and needn't reach their ends.
There are 2 independent parts, one for each index of `group`. The reference program is written for one: setup_inputs(seed, part) draws one part's arguments, and reference() takes and returns one part's arrays. A program takes and returns all parts, laid end to end along the dimension named above; each array names one. Nothing has to cross between parts.
Inputs may be any that keep to these rules, and one draw needn't show every extreme that they name: `kv_lengths`: the longest request holds exactly 32768 tokens. `page_table`: row r lists in order the cache slots of the first ceil(kv_lengths[r] / 128) pages of request r and -1 after them; no slot is listed twice.
All inputs are finite; a program needn't handle non-finite values.
Results may differ from the reference program's by a relative error of at most 0.0042.
Values may be sent and summed in bfloat16 or wider, within the bound.
No kernel may reach another device: no remote copies, remote signals or barrier semaphores. Data moves between devices by JAX's collectives and lax.ppermute only.
A program may use at most 64 MiB of HBM per device.

```python
import jax
import jax.numpy as jnp
from jax import lax

QUERY_HEADS = 64
KEY_VALUE_HEADS = 8
HEAD_WIDTH = 128
PAGE_TOKENS = 128
REQS = 32
POOL_SLOTS = 1024
MAXPAGES = 256


def page_plan(key):
    plan_key = jax.random.fold_in(key, 31)
    key_counts, key_long, key_tail, key_slots = jax.random.split(plan_key, 4)
    request_ids = jnp.arange(REQS, dtype=jnp.int32)
    ceiling = POOL_SLOTS // 4 // (REQS - 1)
    counts = jax.random.randint(key_counts, (REQS,), 1, ceiling + 1, dtype=jnp.int32)
    longest = jax.random.randint(key_long, (), 0, REQS, dtype=jnp.int32)
    counts = jnp.where(request_ids == longest, MAXPAGES, counts).astype(jnp.int32)
    tail_tokens = jax.random.randint(key_tail, (REQS,), 1, PAGE_TOKENS + 1, dtype=jnp.int32)
    lengths = jnp.where(request_ids == longest, MAXPAGES * PAGE_TOKENS, (counts - 1) * PAGE_TOKENS + tail_tokens)
    shuffled = jax.random.permutation(key_slots, POOL_SLOTS).astype(jnp.int32)
    starts = jnp.cumsum(counts) - counts
    page_ids = jnp.arange(MAXPAGES, dtype=jnp.int32)
    slot_index = jnp.clip(starts[:, None] + page_ids[None, :], 0, POOL_SLOTS - 1)
    page_rows = jnp.where(page_ids[None, :] < counts[:, None], jnp.take(shuffled, slot_index), -1)
    return (lengths.astype(jnp.int32), page_rows.astype(jnp.int32))


def draw_kv_lengths(key, part):
    return page_plan(key)[0]


def draw_page_table(key, part):
    return page_plan(key)[1]


def draw_queries(key, part):
    values = jnp.clip(jax.random.normal(jax.random.fold_in(key, 11), (REQS, QUERY_HEADS, HEAD_WIDTH), jnp.float32), -6.0, 6.0)
    return values.astype(jnp.bfloat16)


def draw_k_cache(key, part):
    cache_layout = (POOL_SLOTS, KEY_VALUE_HEADS, PAGE_TOKENS, HEAD_WIDTH)
    values = jnp.clip(jax.random.normal(jax.random.fold_in(key, 13), cache_layout, jnp.float32), -6.0, 6.0)
    return values.astype(jnp.bfloat16)


def shard_levels(stream_key, extent, cuts, low, top_value):
    def one(axis_at, parts):
        steps = jax.random.uniform(jax.random.fold_in(jax.random.fold_in(stream_key, 6), axis_at), (parts,), jnp.float32, low / len(cuts), top_value / len(cuts))
        return jnp.repeat(jnp.exp(steps), extent[axis_at] // parts).reshape((-1,) + (1,) * (len(extent) - axis_at - 1))

    factor_of = one(*cuts[0])
    for cut in cuts[1:]:
        factor_of = factor_of * one(*cut)
    return factor_of


def normal_values(rng, shape, deviation, limit, shards=(), kind=jnp.bfloat16):
    result = jax.random.normal(rng, shape, jnp.float32) * deviation
    if len(shards) > 0:
        result = shard_levels(rng, shape, shards, -0.22, 0.18) * result
    return jnp.clip(result, min=-limit, max=limit).astype(kind)


def setup_inputs(seed: int = 0, part: int = 0) -> dict:
    keys = jax.random.split(jax.random.key(seed), 7)
    part_keys = jax.random.split(jax.random.fold_in(keys[6], part), 7)
    return {
        "queries": draw_queries(jax.random.fold_in(jax.random.fold_in(keys[6], part), 71), part),
        "k_cache": draw_k_cache(jax.random.fold_in(jax.random.fold_in(keys[6], part), 71), part),
        "value_cache": normal_values(part_keys[2], (POOL_SLOTS, KEY_VALUE_HEADS, PAGE_TOKENS, HEAD_WIDTH), 1.0, 6.0, ((0, 128), (1, 2))),
        "kv_lengths": draw_kv_lengths(jax.random.fold_in(jax.random.fold_in(keys[6], part), 71), part),
        "page_table": draw_page_table(jax.random.fold_in(jax.random.fold_in(keys[6], part), 71), part),
        "request_batch_row": jax.random.permutation(part_keys[5], REQS).astype(jnp.int32),
    }


NEG_BIG = -1.0e30


def reference(queries, k_cache, value_cache, kv_lengths, page_table, request_batch_row):
    group_width = QUERY_HEADS // KEY_VALUE_HEADS
    scale = HEAD_WIDTH ** -0.5

    def one_request(request_number):
        slot_rows = jnp.maximum(page_table[request_number], 0).astype(jnp.int32)
        key_pages = jnp.take(k_cache, slot_rows, axis=0).astype(jnp.float32)
        value_pages = jnp.take(value_cache, slot_rows, axis=0).astype(jnp.float32)
        query_head_rows = queries[request_batch_row[request_number]].astype(jnp.float32).reshape(KEY_VALUE_HEADS, group_width, HEAD_WIDTH)
        scores = jnp.einsum("kgd,pktd->pkgt", query_head_rows, key_pages) * scale
        positions = jnp.arange(MAXPAGES * PAGE_TOKENS, dtype=jnp.int32).reshape(MAXPAGES, PAGE_TOKENS)
        valid_mask = (positions < kv_lengths[request_number])[:, None, None, :]
        masked = jnp.where(valid_mask, scores, NEG_BIG)
        page_max = jnp.max(masked, axis=3)
        weights = jnp.where(valid_mask, jnp.exp(masked - page_max[..., None]), 0.0)
        page_sum = jnp.sum(weights, axis=3)
        weights_bf = lax.optimization_barrier(weights.astype(jnp.bfloat16))
        page_out = jnp.einsum("pkgt,pktd->pkgd", weights_bf.astype(jnp.float32), value_pages)
        request_top = jnp.max(page_max, axis=0)
        factor = jnp.exp(page_max - request_top[None])
        total_sum = jnp.sum(page_sum * factor, axis=0)
        total_out = jnp.sum(page_out * factor[..., None], axis=0)
        return (total_out / total_sum[..., None]).astype(jnp.bfloat16).reshape(QUERY_HEADS, HEAD_WIDTH)

    results = lax.map(one_request, jnp.arange(REQS, dtype=jnp.int32))
    return jnp.zeros((REQS, QUERY_HEADS, HEAD_WIDTH), jnp.bfloat16).at[request_batch_row].set(results)
```

```python
import functools

import jax
import jax.numpy as jnp
from jax import lax
from jax.experimental import pallas as pl
from jax.experimental.pallas import tpu as pltpu
from jax.sharding import Mesh
from jax.sharding import PartitionSpec as P

NEG_BIG = -1e30
SIDE = 4
BLOCK = ("near", "across")
SEQ = ("far", "near", "across")
GROUP_SEQ = ("group", "far", "near", "across")
STAT_ROWS = 8
STAT_ROWS_BF = 16


def attend_kernel(
    place, batch_row, lengths, table, queries, k_hbm, v_hbm, out, k_buf, v_buf, rows, stats, sems
):
    slots, heads_kv, page_len, width = k_buf.shape
    heads = queries.shape[1]
    group = heads // heads_kv
    peers = out.shape[0]
    share = heads // peers
    max_pages = table.shape[1]

    def k_copy(s):
        return pltpu.make_async_copy(k_hbm.at[s], k_buf.at[s], sems.at[0, s])

    def v_copy(s):
        return pltpu.make_async_copy(v_hbm.at[s], v_buf.at[s], sems.at[1, s])

    for s in range(slots):
        k_copy(s).start()
    for s in range(slots):
        v_copy(s).start()

    first_slot = place[0]
    first_lane = place[1]
    lane = lax.broadcasted_iota(jnp.int32, (heads, page_len), 1)
    entry = table[...]
    code = (
        lax.broadcasted_iota(jnp.int32, entry.shape, 0) * max_pages
        + lax.broadcasted_iota(jnp.int32, entry.shape, 1)
        + 1
    ).astype(jnp.float32)
    owner_row = jnp.zeros((STAT_ROWS // 2, page_len), jnp.float32)
    slot_queries = []
    valid_count = []
    for s in range(slots):
        found = jnp.max(jnp.where(entry == first_slot + s, code, 0.0)).astype(jnp.int32)
        index = jnp.maximum(found - 1, 0)
        request = index // max_pages
        page = index % max_pages
        row = batch_row[request]
        left = jnp.where(found > 0, lengths[request] - page * page_len, 0)
        valid_count.append(left)
        slot_queries.append(row)
        marked = jnp.where(found > 0, row + 1, 0).astype(jnp.float32)
        owner_row = jnp.where(
            lane[: STAT_ROWS // 2] == first_lane + s, marked, owner_row
        )

    scale = width ** (-0.5)
    max_rows = jnp.zeros((heads, page_len), jnp.float32)
    sum_rows = jnp.zeros((heads, page_len), jnp.float32)
    weights = []
    for s in range(slots):
        k_copy(s).wait()
        q = queries[slot_queries[s]]
        parts = []
        for k in range(heads_kv):
            full = lax.dot_general(
                q, k_buf[s, k], (((1,), (1,)), ((), ())), preferred_element_type=jnp.float32
            )
            parts.append(full[k * group : (k + 1) * group])
        valid = lane < valid_count[s]
        scores = jnp.where(valid, jnp.concatenate(parts, axis=0) * scale, NEG_BIG)
        top = jnp.max(scores, axis=1, keepdims=True)
        weight = jnp.where(valid, jnp.exp(scores - top), 0.0)
        total = jnp.sum(weight, axis=1, keepdims=True)
        mine = lane == first_lane + s
        max_rows = jnp.where(mine, top, max_rows)
        sum_rows = jnp.where(mine, total, sum_rows)
        weights.append(weight.astype(jnp.bfloat16))
    for s in range(slots):
        v_copy(s).wait()
        for k in range(heads_kv):
            full = jnp.dot(weights[s], v_buf[s, k], preferred_element_type=jnp.float32)
            rows[s * heads + k * group : s * heads + (k + 1) * group] = full[
                k * group : (k + 1) * group
            ]
    stats[:heads] = max_rows
    stats[heads:] = sum_rows
    for p in range(peers):
        for h in range(share):
            out[p, h * slots : (h + 1) * slots] = rows[pl.ds(p * share + h, slots, stride=heads)]
        first = p * share
        out[p, share * slots :] = jnp.concatenate(
            [stats[first : first + share], stats[heads + first : heads + first + share], owner_row],
            axis=0,
        )


def pieces_of(x):
    high = x.astype(jnp.bfloat16).astype(jnp.float32)
    rest = x - high
    middle = rest.astype(jnp.bfloat16).astype(jnp.float32)
    return high, middle, rest - middle


def merge_slots_kernel(got, out):
    peers, height, width = got.shape
    blocks, out_height, _ = out.shape
    slots = (height - STAT_ROWS) // 2
    share = 2
    requests = (out_height - STAT_ROWS_BF) // share
    stat = got[0, share * slots :]
    for i in range(1, peers):
        stat = stat + got[i, share * slots :]
    owner = stat[2 * share : 2 * share + 1].astype(jnp.int32) - 1
    owned = owner == lax.broadcasted_iota(jnp.int32, (requests, width), 0)
    tops = []
    totals = []
    for h in range(share):
        data = got[:, h * slots : (h + 1) * slots].reshape(peers * slots, width)
        slot_top = stat[h : h + 1]
        top = jnp.max(jnp.where(owned, slot_top, NEG_BIG), axis=1, keepdims=True)
        factor = jnp.where(owned, jnp.exp(slot_top - top), 0.0)
        total = jnp.sum(factor * stat[share + h : share + h + 1], axis=1, keepdims=True)
        merged = jnp.dot(
            factor, data, precision=lax.Precision.HIGHEST, preferred_element_type=jnp.float32
        )
        scaled = jnp.where(total > 0.0, merged / jnp.where(total > 0.0, total, 1.0), 0.0)
        scaled = scaled.astype(jnp.bfloat16)
        for j in range(blocks):
            out[j, h * requests : (h + 1) * requests] = scaled
        tops.append(top)
        totals.append(total)
    lane = lax.broadcasted_iota(jnp.int32, (share * requests, width), 1)
    table = jnp.zeros((share * requests, width), jnp.float32)
    columns = zip(
        pieces_of(jnp.concatenate(tops, axis=0)), pieces_of(jnp.concatenate(totals, axis=0))
    )
    for n, (top, total) in enumerate(columns):
        table = jnp.where(lane == 2 * n, top, table)
        table = jnp.where(lane == 2 * n + 1, total, table)
    square = jnp.concatenate(
        [table, jnp.zeros((width - share * requests, width), jnp.float32)], axis=0
    )
    tile = jnp.transpose(square)[:STAT_ROWS_BF].astype(jnp.bfloat16)
    for j in range(blocks):
        out[j, share * requests :] = tile


def merge_blocks_kernel(got, out):
    blocks, height, width = got.shape
    peers = out.shape[0]
    count = height - STAT_ROWS_BF
    tops = []
    totals = []
    for j in range(blocks):
        tile = got[j, count:].astype(jnp.float32)
        tops.append(tile[0:1] + tile[2:3] + tile[4:5])
        totals.append(tile[1:2] + tile[3:4] + tile[5:6])
    top = jnp.concatenate(tops, axis=0)
    total = jnp.concatenate(totals, axis=0)
    share = jnp.exp(top - jnp.max(top, axis=0, keepdims=True)) * total
    whole = jnp.sum(share, axis=0, keepdims=True)
    share = jnp.where(whole > 0.0, share / jnp.where(whole > 0.0, whole, 1.0), 0.0)
    square = jnp.concatenate([share, jnp.zeros((width - blocks, width), jnp.float32)], axis=0)
    column = jnp.transpose(square)[:count]
    result = column[:, 0:1] * got[0, :count].astype(jnp.float32)
    for j in range(1, blocks):
        result = result + column[:, j : j + 1] * got[j, :count].astype(jnp.float32)
    result = result.astype(jnp.bfloat16)
    for p in range(peers):
        out[p] = result


def in_vmem():
    return pl.BlockSpec(memory_space=pltpu.VMEM)


def in_smem():
    return pl.BlockSpec(memory_space=pltpu.SMEM)


def shards(blocks, queries, k_cache, value_cache, kv_lengths, page_table, request_batch_row):
    slots, heads_kv, page_len, width = k_cache.shape
    requests, heads, _ = queries.shape
    peers = SIDE * SIDE
    share = heads // peers
    place = jnp.stack(
        [lax.axis_index(SEQ) * slots, lax.axis_index(BLOCK) * slots]
    ).astype(jnp.int32)
    partial = pl.pallas_call(
        attend_kernel,
        out_shape=jax.ShapeDtypeStruct((peers, share * slots + STAT_ROWS, width), jnp.float32),
        in_specs=[in_smem(), in_smem(), in_smem(), in_vmem(), in_vmem()]
        + [pl.BlockSpec(memory_space=pl.ANY)] * 2,
        out_specs=in_vmem(),
        scratch_shapes=[
            pltpu.VMEM(k_cache.shape, k_cache.dtype),
            pltpu.VMEM(value_cache.shape, value_cache.dtype),
            pltpu.VMEM((slots * heads, width), jnp.float32),
            pltpu.VMEM((2 * heads, page_len), jnp.float32),
            pltpu.SemaphoreType.DMA((2, slots)),
        ],
        name="attend",
    )(place, request_batch_row, kv_lengths, page_table, queries, k_cache, value_cache)
    partial = lax.all_to_all(partial, BLOCK, 0, 0)
    merged = pl.pallas_call(
        merge_slots_kernel,
        out_shape=jax.ShapeDtypeStruct(
            (blocks, share * requests + STAT_ROWS_BF, width), jnp.bfloat16
        ),
        in_specs=[in_vmem()],
        out_specs=in_vmem(),
        name="merge_slots",
    )(partial)
    merged = lax.all_to_all(merged, "far", 0, 0)
    finished = pl.pallas_call(
        merge_blocks_kernel,
        out_shape=jax.ShapeDtypeStruct((peers, share * requests, width), jnp.bfloat16),
        in_specs=[in_vmem()],
        out_specs=in_vmem(),
        name="merge_blocks",
    )(merged)
    finished = lax.all_to_all(finished, BLOCK, 0, 0)
    return finished.reshape(heads, requests, width).transpose(1, 0, 2)


def solution(mesh):
    blocks = mesh.shape["seq"] // (SIDE * SIDE)
    finer = Mesh(
        mesh.devices.reshape(mesh.shape["group"], blocks, SIDE, SIDE, mesh.shape["tensor"]),
        ("group", "far", "near", "across", "tensor"),
    )
    placed = (
        P("group", "tensor", None),
        P(GROUP_SEQ, "tensor", None, None),
        P(GROUP_SEQ, "tensor", None, None),
        P("group"),
        P("group", None),
        P("group"),
    )
    return jax.shard_map(
        functools.partial(shards, blocks),
        mesh=finer,
        in_specs=placed,
        out_specs=P("group", "tensor", None),
        check_vma=False,
    )
```

```python
import functools

import jax
import jax.numpy as jnp
from jax import lax
from jax.experimental import pallas as pl
from jax.experimental.pallas import tpu as pltpu
from jax.sharding import Mesh
from jax.sharding import PartitionSpec as P

NEG_BIG = -1e30
SIDE = 4
BLOCK = ("near", "across")
SEQ = ("far", "near", "across")
GROUP_SEQ = ("group", "far", "near", "across")
STAT_ROWS = 8
PIECES = 3
BATCH = 4
ROOT = 1


def attend_kernel(
    batch_row_hbm,
    lengths_hbm,
    table_hbm,
    queries_hbm,
    k_hbm,
    v_hbm,
    out,
    batch_row,
    lengths,
    table,
    queries,
    k_buf,
    v_buf,
    rows,
    stats,
    sems,
    small_sems,
):
    slots, heads_kv, page_len, width = k_buf.shape
    heads = queries.shape[1]
    group = heads // heads_kv
    peers = out.shape[0]
    share = heads // peers
    max_pages = table.shape[1]

    def k_copy(s):
        return pltpu.make_async_copy(k_hbm.at[s], k_buf.at[s], sems.at[0, s])

    def v_copy(s):
        return pltpu.make_async_copy(v_hbm.at[s], v_buf.at[s], sems.at[1, s])

    small = [
        pltpu.make_async_copy(source, target, small_sems.at[n])
        for n, (source, target) in enumerate(
            [
                (table_hbm, table),
                (batch_row_hbm, batch_row),
                (lengths_hbm, lengths),
                (queries_hbm, queries),
            ]
        )
    ]
    for copy in small:
        copy.start()
    @pl.loop(0, slots)
    def _(s):
        k_copy(s).start()

    @pl.loop(0, slots)
    def _(s):
        v_copy(s).start()

    first_slot = lax.axis_index(SEQ) * slots
    first_lane = lax.axis_index(BLOCK) * slots
    lane = lax.broadcasted_iota(jnp.int32, (heads, page_len), 1)
    for copy in small:
        copy.wait()
    entry = table[...]
    code = (
        lax.broadcasted_iota(jnp.int32, entry.shape, 0) * max_pages
        + lax.broadcasted_iota(jnp.int32, entry.shape, 1)
        + 1
    ).astype(jnp.float32)
    owner_rows = STAT_ROWS - PIECES * share
    owner_row = jnp.zeros((owner_rows, page_len), jnp.float32)
    slot_queries = []
    valid_count = []
    for s in range(slots):
        found = jnp.max(jnp.where(entry == first_slot + s, code, 0.0)).astype(jnp.int32)
        index = jnp.maximum(found - 1, 0)
        request = index // max_pages
        page = index % max_pages
        row = batch_row[request]
        left = jnp.where(found > 0, lengths[request] - page * page_len, 0)
        valid_count.append(left)
        slot_queries.append(row)
        marked = jnp.where(found > 0, row + 1, 0).astype(jnp.float32)
        owner_row = jnp.where(lane[:owner_rows] == first_lane + s, marked, owner_row)

    scale = width ** (-0.5)
    level_rows = jnp.zeros((heads, page_len), jnp.float32)
    weights = []
    inverses = []
    for s in range(slots):
        if s % BATCH == 0:
            for n in range(s, s + BATCH):
                k_copy(n).wait()
        q = queries[slot_queries[s]]
        parts = []
        for k in range(heads_kv):
            full = lax.dot_general(
                q, k_buf[s, k], (((1,), (1,)), ((), ())), preferred_element_type=jnp.float32
            )
            parts.append(full[k * group : (k + 1) * group])
        valid = lane < valid_count[s]
        scores = jnp.where(valid, jnp.concatenate(parts, axis=0) * scale, NEG_BIG)
        top = jnp.max(scores, axis=1, keepdims=True)
        weight = jnp.where(valid, jnp.exp(scores - top), 0.0)
        total = jnp.sum(weight, axis=1, keepdims=True)
        live = total > 0.0
        total = jnp.where(live, total, 1.0)
        level = jnp.where(live, top + jnp.log(total), NEG_BIG)
        level_rows = jnp.where(lane == first_lane + s, level, level_rows)
        weights.append(weight.astype(jnp.bfloat16))
        inverses.append(1.0 / total)
    for s in range(slots):
        if s % BATCH == 0:
            for n in range(s, s + BATCH):
                v_copy(n).wait()
        for k in range(heads_kv):
            full = jnp.dot(weights[s], v_buf[s, k], preferred_element_type=jnp.float32)
            lines = slice(k * group, (k + 1) * group)
            rows[s * heads + k * group : s * heads + (k + 1) * group] = (
                full[lines] * inverses[s][lines]
            )
    for n, piece in enumerate(pieces_of(level_rows)):
        stats[n * heads : (n + 1) * heads] = piece
    for p in range(peers):
        for h in range(share):
            line = rows[pl.ds(p * share + h, slots, stride=heads)]
            out[p, h * slots : (h + 1) * slots] = line.astype(jnp.bfloat16)
        first = p * share
        lines = [stats[n * heads + first : n * heads + first + share] for n in range(PIECES)]
        out[p, share * slots :] = jnp.concatenate(lines + [owner_row], axis=0).astype(jnp.bfloat16)


def pieces_of(x):
    high = x.astype(jnp.bfloat16).astype(jnp.float32)
    rest = x - high
    middle = rest.astype(jnp.bfloat16).astype(jnp.float32)
    return high, middle, (rest - middle).astype(jnp.bfloat16).astype(jnp.float32)


def merge_slots_kernel(got, out):
    peers, height, width = got.shape
    slots = (height - STAT_ROWS) // 2
    share = 2
    requests = (out.shape[0] - STAT_ROWS) // share
    stat = got[0, share * slots :].astype(jnp.float32)
    for i in range(1, peers):
        stat = stat + got[i, share * slots :].astype(jnp.float32)
    owner = stat[PIECES * share : PIECES * share + 1].astype(jnp.int32) - 1
    owned = owner == lax.broadcasted_iota(jnp.int32, (requests, width), 0)
    levels = []
    for h in range(share):
        data = got[:, h * slots : (h + 1) * slots].astype(jnp.float32).reshape(peers * slots, width)
        level = stat[h : h + 1] + stat[share + h : share + h + 1]
        level = level + stat[2 * share + h : 2 * share + h + 1]
        top = jnp.max(jnp.where(owned, level, NEG_BIG), axis=1, keepdims=True)
        factor = jnp.where(owned, jnp.exp(level - top), 0.0)
        total = jnp.sum(factor, axis=1, keepdims=True)
        merged = jnp.dot(
            factor, data, precision=lax.Precision.HIGHEST, preferred_element_type=jnp.float32
        )
        live = total > 0.0
        total = jnp.where(live, total, 1.0)
        out[h * requests : (h + 1) * requests] = (merged / total).astype(jnp.bfloat16)
        levels.append(jnp.where(live, top + jnp.log(total), NEG_BIG))
    lane = lax.broadcasted_iota(jnp.int32, (share * requests, width), 1)
    table = jnp.zeros((share * requests, width), jnp.float32)
    for n, piece in enumerate(pieces_of(jnp.concatenate(levels, axis=0))):
        table = jnp.where(lane == n, piece, table)
    square = jnp.concatenate(
        [table, jnp.zeros((width - share * requests, width), jnp.float32)], axis=0
    )
    out[share * requests :] = jnp.transpose(square)[:STAT_ROWS].astype(jnp.bfloat16)


def merge_blocks_kernel(*refs):
    *got, out = refs
    blocks = len(got)
    height, width = got[0].shape
    count = height - STAT_ROWS
    levels = []
    for j in range(blocks):
        tile = got[j][count:].astype(jnp.float32)
        levels.append(tile[0:1] + tile[1:2] + tile[2:3])
    level = jnp.concatenate(levels, axis=0)
    share = jnp.exp(level - jnp.max(level, axis=0, keepdims=True))
    share = share / jnp.sum(share, axis=0, keepdims=True)
    square = jnp.concatenate([share, jnp.zeros((width - blocks, width), jnp.float32)], axis=0)
    column = jnp.transpose(square)[:count]
    result = column[:, 0:1] * got[0][:count].astype(jnp.float32)
    for j in range(1, blocks):
        result = result + column[:, j : j + 1] * got[j][:count].astype(jnp.float32)
    out[...] = result.astype(jnp.bfloat16)


def spread_kernel(order, *refs):
    *sent, out = refs
    block = lax.axis_index("far")
    for which, ref in zip(order, sent):

        @pl.when(block == which)
        def _(ref=ref):
            row = ref[...]
            for p in range(out.shape[0]):
                out[p] = row


def in_vmem():
    return pl.BlockSpec(memory_space=pltpu.VMEM)


def kept(shape, dtype):
    return pltpu.VMEM(shape, dtype)


def near(x):
    return pltpu.with_memory_space_constraint(x, pltpu.VMEM)


def shards(blocks, queries, k_cache, value_cache, kv_lengths, page_table, request_batch_row):
    slots, heads_kv, page_len, width = k_cache.shape
    requests, heads, _ = queries.shape
    peers = SIDE * SIDE
    share = heads // peers
    partial = pl.pallas_call(
        attend_kernel,
        out_shape=kept((peers, share * slots + STAT_ROWS, width), jnp.bfloat16),
        in_specs=[pl.BlockSpec(memory_space=pl.ANY)] * 6,
        out_specs=in_vmem(),
        scratch_shapes=[
            pltpu.SMEM(request_batch_row.shape, jnp.int32),
            pltpu.SMEM(kv_lengths.shape, jnp.int32),
            pltpu.VMEM(page_table.shape, jnp.int32),
            pltpu.VMEM(queries.shape, queries.dtype),
            pltpu.VMEM(k_cache.shape, k_cache.dtype),
            pltpu.VMEM(value_cache.shape, value_cache.dtype),
            pltpu.VMEM((slots * heads, width), jnp.float32),
            pltpu.VMEM((PIECES * heads, page_len), jnp.float32),
            pltpu.SemaphoreType.DMA((2, slots)),
            pltpu.SemaphoreType.DMA((4,)),
        ],
        name="attend",
    )(request_batch_row, kv_lengths, page_table, queries, k_cache, value_cache)
    partial = lax.all_to_all(partial, BLOCK, 0, 0)
    merged = pl.pallas_call(
        merge_slots_kernel,
        out_shape=kept((share * requests + STAT_ROWS, width), jnp.bfloat16),
        in_specs=[in_vmem()],
        out_specs=in_vmem(),
        name="merge_slots",
    )(near(partial))
    others = [(ROOT + n) % blocks for n in range(1, blocks)]
    pieces = [merged] + [lax.ppermute(merged, "far", [(j, ROOT)]) for j in others]
    result = pl.pallas_call(
        merge_blocks_kernel,
        out_shape=kept((share * requests, width), jnp.bfloat16),
        in_specs=[in_vmem()] * blocks,
        out_specs=in_vmem(),
        name="merge_blocks",
    )(*[near(piece) for piece in pieces])
    order = [ROOT] + others
    sent = [result] + [lax.ppermute(result, "far", [(ROOT, j)]) for j in others]
    finished = pl.pallas_call(
        functools.partial(spread_kernel, order),
        out_shape=kept((peers, share * requests, width), jnp.bfloat16),
        in_specs=[in_vmem()] * blocks,
        out_specs=in_vmem(),
        name="spread",
    )(*[near(piece) for piece in sent])
    finished = lax.all_to_all(finished, BLOCK, 0, 0)
    return finished.reshape(heads, requests, width).transpose(1, 0, 2)


def solution(mesh):
    blocks = mesh.shape["seq"] // (SIDE * SIDE)
    finer = Mesh(
        mesh.devices.reshape(mesh.shape["group"], blocks, SIDE, SIDE, mesh.shape["tensor"]),
        ("group", "far", "near", "across", "tensor"),
    )
    placed = (
        P("group", "tensor", None),
        P(GROUP_SEQ, "tensor", None, None),
        P(GROUP_SEQ, "tensor", None, None),
        P("group"),
        P("group", None),
        P("group"),
    )
    return jax.shard_map(
        functools.partial(shards, blocks),
        mesh=finer,
        in_specs=placed,
        out_specs=P("group", "tensor", None),
        check_vma=False,
    )
```

```python
import functools

import jax
import jax.numpy as jnp
from jax import lax
from jax.experimental import pallas as pl
from jax.experimental.pallas import tpu as pltpu
from jax.sharding import Mesh
from jax.sharding import PartitionSpec as P

NEG_BIG = -1e30
ACROSS = 4
NEAR = 2
BLOCK = ("near", "across")
SEQ = ("far", "near", "across")
GROUP_SEQ = ("group", "far", "near", "across")
PIECES = 3
STAT_ROWS = 8
HUBS = (2, 10, 13, 6)
BATCH = 4
ROOT = 1


def attend_kernel(
    batch_row_hbm,
    lengths_hbm,
    table_hbm,
    queries_hbm,
    k_hbm,
    v_hbm,
    out,
    batch_row,
    lengths,
    table,
    queries,
    k_buf,
    v_buf,
    rows,
    stats,
    sems,
    small_sems,
):
    slots, heads_kv, page_len, width = k_buf.shape
    heads = queries.shape[1]
    group = heads // heads_kv
    peers = out.shape[0]
    share = heads // peers
    max_pages = table.shape[1]

    def k_copy(s):
        return pltpu.make_async_copy(k_hbm.at[s], k_buf.at[s], sems.at[0, s])

    def v_copy(s):
        return pltpu.make_async_copy(v_hbm.at[s], v_buf.at[s], sems.at[1, s])

    small = [
        pltpu.make_async_copy(source, target, small_sems.at[n])
        for n, (source, target) in enumerate(
            [
                (table_hbm, table),
                (batch_row_hbm, batch_row),
                (lengths_hbm, lengths),
                (queries_hbm, queries),
            ]
        )
    ]
    for copy in small:
        copy.start()
    @pl.loop(0, slots)
    def _(s):
        k_copy(s).start()

    @pl.loop(0, slots)
    def _(s):
        v_copy(s).start()

    first_slot = lax.axis_index(SEQ) * slots
    first_lane = lax.axis_index(BLOCK) * slots
    lane = lax.broadcasted_iota(jnp.int32, (heads, page_len), 1)
    for copy in small:
        copy.wait()
    entry = table[...]
    code = (
        lax.broadcasted_iota(jnp.int32, entry.shape, 0) * max_pages
        + lax.broadcasted_iota(jnp.int32, entry.shape, 1)
        + 1
    ).astype(jnp.float32)
    owner_rows = out.shape[1] - (slots + PIECES) * share
    owner_row = jnp.zeros((owner_rows, page_len), jnp.float32)
    slot_queries = []
    valid_count = []
    for s in range(slots):
        found = jnp.max(jnp.where(entry == first_slot + s, code, 0.0)).astype(jnp.int32)
        index = jnp.maximum(found - 1, 0)
        request = index // max_pages
        page = index % max_pages
        row = batch_row[request]
        left = jnp.where(found > 0, lengths[request] - page * page_len, 0)
        valid_count.append(left)
        slot_queries.append(row)
        marked = jnp.where(found > 0, row + 1, 0).astype(jnp.float32)
        owner_row = jnp.where(lane[:owner_rows] == first_lane + s, marked, owner_row)

    scale = width ** (-0.5)
    level_rows = jnp.zeros((heads, page_len), jnp.float32)
    weights = []
    inverses = []
    for s in range(slots):
        if s % BATCH == 0:
            for n in range(s, s + BATCH):
                k_copy(n).wait()
        q = queries[slot_queries[s]]
        parts = []
        for k in range(heads_kv):
            full = lax.dot_general(
                q, k_buf[s, k], (((1,), (1,)), ((), ())), preferred_element_type=jnp.float32
            )
            parts.append(full[k * group : (k + 1) * group])
        valid = lane < valid_count[s]
        scores = jnp.where(valid, jnp.concatenate(parts, axis=0) * scale, NEG_BIG)
        top = jnp.max(scores, axis=1, keepdims=True)
        weight = jnp.where(valid, jnp.exp(scores - top), 0.0)
        total = jnp.sum(weight, axis=1, keepdims=True)
        live = total > 0.0
        total = jnp.where(live, total, 1.0)
        level = jnp.where(live, top + jnp.log(total), NEG_BIG)
        level_rows = jnp.where(lane == first_lane + s, level, level_rows)
        weights.append(weight.astype(jnp.bfloat16))
        inverses.append(1.0 / total)
    for s in range(slots):
        if s % BATCH == 0:
            for n in range(s, s + BATCH):
                v_copy(n).wait()
        for k in range(heads_kv):
            full = jnp.dot(weights[s], v_buf[s, k], preferred_element_type=jnp.float32)
            lines = slice(k * group, (k + 1) * group)
            rows[s * heads + k * group : s * heads + (k + 1) * group] = (
                full[lines] * inverses[s][lines]
            )
    for n, piece in enumerate(pieces_of(level_rows)):
        stats[n * heads : (n + 1) * heads] = piece
    for p in range(peers):
        for h in range(share):
            line = rows[pl.ds(p * share + h, slots, stride=heads)]
            out[p, h * slots : (h + 1) * slots] = line.astype(jnp.bfloat16)
        first = p * share
        lines = [stats[n * heads + first : n * heads + first + share] for n in range(PIECES)]
        out[p, share * slots :] = jnp.concatenate(lines + [owner_row], axis=0).astype(jnp.bfloat16)


def pieces_of(x):
    high = x.astype(jnp.bfloat16).astype(jnp.float32)
    rest = x - high
    middle = rest.astype(jnp.bfloat16).astype(jnp.float32)
    return high, middle, (rest - middle).astype(jnp.bfloat16).astype(jnp.float32)


def merge_slots_kernel(share, slots, got, out):
    peers, height, width = got.shape
    count = peers * slots
    requests = (out.shape[0] - STAT_ROWS) // share
    stat = got[0, share * slots :].astype(jnp.float32)
    for i in range(1, peers):
        stat = stat + got[i, share * slots :].astype(jnp.float32)
    owner = stat[PIECES * share : PIECES * share + 1].astype(jnp.int32) - 1
    owned = owner == lax.broadcasted_iota(jnp.int32, (requests, width), 0)
    levels = []
    for h in range(share):
        data = got[:, h * slots : (h + 1) * slots].astype(jnp.float32).reshape(count, width)
        level = stat[h : h + 1] + stat[share + h : share + h + 1]
        level = level + stat[2 * share + h : 2 * share + h + 1]
        top = jnp.max(jnp.where(owned, level, NEG_BIG), axis=1, keepdims=True)
        factor = jnp.where(owned, jnp.exp(level - top), 0.0)
        total = jnp.sum(factor, axis=1, keepdims=True)
        merged = jnp.dot(
            factor[:, :count], data, precision=lax.Precision.HIGHEST, preferred_element_type=jnp.float32
        )
        live = total > 0.0
        total = jnp.where(live, total, 1.0)
        out[h * requests : (h + 1) * requests] = (merged / total).astype(jnp.bfloat16)
        levels.append(jnp.where(live, top + jnp.log(total), NEG_BIG))
    lane = lax.broadcasted_iota(jnp.int32, (share * requests, width), 1)
    table = jnp.zeros((share * requests, width), jnp.float32)
    for n, piece in enumerate(pieces_of(jnp.concatenate(levels, axis=0))):
        table = jnp.where(lane == n, piece, table)
    out[share * requests :] = jnp.transpose(table)[:STAT_ROWS].astype(jnp.bfloat16)


def merge_blocks_kernel(*refs):
    *got, out = refs
    blocks = len(got)
    height, width = got[0].shape
    count = height - STAT_ROWS
    levels = []
    for j in range(blocks):
        tile = got[j][count:].astype(jnp.float32)
        levels.append(tile[0:1] + tile[1:2] + tile[2:3])
    level = jnp.concatenate(levels, axis=0)
    share = jnp.exp(level - jnp.max(level, axis=0, keepdims=True))
    share = share / jnp.sum(share, axis=0, keepdims=True)
    square = jnp.concatenate([share, jnp.zeros((width - blocks, width), jnp.float32)], axis=0)
    column = jnp.transpose(square)[:count]
    result = column[:, 0:1] * got[0][:count].astype(jnp.float32)
    for j in range(1, blocks):
        result = result + column[:, j : j + 1] * got[j][:count].astype(jnp.float32)
    out[...] = result.astype(jnp.bfloat16)


def pick_kernel(holders, *refs):
    *sent, out = refs
    block = lax.axis_index("far")
    for members, ref in zip(holders, sent):
        here = functools.reduce(jnp.logical_or, [block == j for j in members])

        @pl.when(here)
        def _(ref=ref):
            row = ref[...]
            if len(out.shape) == len(ref.shape):
                out[...] = row
            else:
                for p in range(out.shape[0]):
                    out[p] = row


def in_vmem():
    return pl.BlockSpec(memory_space=pltpu.VMEM)


def kept(shape, dtype):
    return pltpu.VMEM(shape, dtype)


def near(x):
    return pltpu.with_memory_space_constraint(x, pltpu.VMEM)


def shards(blocks, queries, k_cache, value_cache, kv_lengths, page_table, request_batch_row):
    slots, heads_kv, page_len, width = k_cache.shape
    requests, heads, _ = queries.shape
    peers = NEAR * ACROSS
    lines = -(-((slots + PIECES) * (heads // peers) + 1) // 8) * 8
    share = heads // peers
    partial = pl.pallas_call(
        attend_kernel,
        out_shape=kept((peers, lines, width), jnp.bfloat16),
        in_specs=[pl.BlockSpec(memory_space=pl.ANY)] * 6,
        out_specs=in_vmem(),
        scratch_shapes=[
            pltpu.SMEM(request_batch_row.shape, jnp.int32),
            pltpu.SMEM(kv_lengths.shape, jnp.int32),
            pltpu.VMEM(page_table.shape, jnp.int32),
            pltpu.VMEM(queries.shape, queries.dtype),
            pltpu.VMEM(k_cache.shape, k_cache.dtype),
            pltpu.VMEM(value_cache.shape, value_cache.dtype),
            pltpu.VMEM((slots * heads, width), jnp.float32),
            pltpu.VMEM((PIECES * heads, page_len), jnp.float32),
            pltpu.SemaphoreType.DMA((2, slots)),
            pltpu.SemaphoreType.DMA((4,)),
        ],
        name="attend",
    )(request_batch_row, kv_lengths, page_table, queries, k_cache, value_cache)
    partial = lax.all_to_all(partial, BLOCK, 0, 0)
    merged = pl.pallas_call(
        functools.partial(merge_slots_kernel, share, slots),
        out_shape=kept((share * requests + STAT_ROWS, width), jnp.bfloat16),
        in_specs=[in_vmem()],
        out_specs=in_vmem(),
        name="merge_slots",
    )(near(partial))
    def send(x, pairs):
        return lax.ppermute(x, "far", pairs)

    half = ROOT + blocks // 2
    late = sorted(range(half, blocks), key=lambda j: abs(2 * j - half - blocks))
    sources = [*late, ROOT - 1, *range(half - 1, ROOT, -1)]
    pieces = [merged] + [send(merged, [(j, ROOT)]) for j in reversed(sources)]
    result = pl.pallas_call(
        merge_blocks_kernel,
        out_shape=kept((share * requests, width), jnp.bfloat16),
        in_specs=[in_vmem()] * blocks,
        out_specs=in_vmem(),
        name="merge_blocks",
    )(*[near(piece) for piece in pieces])
    first = (ROOT - 1, *HUBS)
    rest = [j for j in range(blocks) if j != ROOT and j not in first]
    turns = -(-len(rest) // len(HUBS))
    second = [
        [(hub, j) for hub, j in zip(HUBS, rest[k::turns])] for k in range(turns)
    ]
    sent = [result] + [send(result, [(ROOT, j)]) for j in reversed(first)]
    holders = [(ROOT,)] + [(j,) for j in reversed(first)]
    result = pl.pallas_call(
        functools.partial(pick_kernel, holders),
        out_shape=kept((share * requests, width), jnp.bfloat16),
        in_specs=[in_vmem()] * len(sent),
        out_specs=in_vmem(),
        name="pick",
    )(*[near(piece) for piece in sent])
    sent = [result] + [send(result, pairs) for pairs in second]
    holders = [(ROOT, *first)] + [tuple(j for _, j in pairs) for pairs in second]
    finished = pl.pallas_call(
        functools.partial(pick_kernel, holders),
        out_shape=kept((peers, share * requests, width), jnp.bfloat16),
        in_specs=[in_vmem()] * len(sent),
        out_specs=in_vmem(),
        name="spread",
    )(*[near(piece) for piece in sent])
    finished = lax.all_to_all(finished, BLOCK, 0, 0)
    return finished.reshape(heads, requests, width).transpose(1, 0, 2)


def solution(mesh):
    blocks = mesh.shape["seq"] // (NEAR * ACROSS)
    finer = Mesh(
        mesh.devices.reshape(mesh.shape["group"], blocks, NEAR, ACROSS, mesh.shape["tensor"]),
        ("group", "far", "near", "across", "tensor"),
    )
    placed = (
        P("group", "tensor", None),
        P(GROUP_SEQ, "tensor", None, None),
        P(GROUP_SEQ, "tensor", None, None),
        P("group"),
        P("group", None),
        P("group"),
    )
    return jax.shard_map(
        functools.partial(shards, blocks),
        mesh=finer,
        in_specs=placed,
        out_specs=P("group", "tensor", None),
        check_vma=False,
    )
```

```python
import functools

import jax
import jax.numpy as jnp
from jax import lax
from jax.experimental import pallas as pl
from jax.experimental.pallas import tpu as pltpu
from jax.sharding import Mesh
from jax.sharding import PartitionSpec as P

NEG_BIG = -1e30
ACROSS = 4
NEAR = 2
BLOCK = ("near", "across")
SEQ = ("far", "near", "across")
GROUP_SEQ = ("group", "far", "near", "across")
PIECES = 3
STAT_ROWS = 8
FIRST = (0, 2, 10, 13, 6)
TURNS = (
    ((2, 3), (10, 12), (13, 14), (6, 8)),
    ((3, 4), (6, 5), (8, 7), (10, 9), (12, 11), (14, 15)),
)
BATCH = 8
ROOT = 1


def attend_kernel(
    batch_row_hbm,
    lengths_hbm,
    table_hbm,
    queries_hbm,
    k_hbm,
    v_hbm,
    out,
    batch_row,
    lengths,
    table,
    queries,
    k_buf,
    v_buf,
    rows,
    stats,
    sems,
    small_sems,
):
    slots, heads_kv, page_len, width = k_buf.shape
    heads = queries.shape[1]
    group = heads // heads_kv
    peers = out.shape[0]
    share = heads // peers
    max_pages = table.shape[1]

    def k_copy(s):
        return pltpu.make_async_copy(k_hbm.at[s], k_buf.at[s], sems.at[0, s])

    def v_copy(s):
        return pltpu.make_async_copy(v_hbm.at[s], v_buf.at[s], sems.at[1, s])

    small = [
        pltpu.make_async_copy(source, target, small_sems.at[n])
        for n, (source, target) in enumerate(
            [
                (table_hbm, table),
                (batch_row_hbm, batch_row),
                (lengths_hbm, lengths),
                (queries_hbm, queries),
            ]
        )
    ]
    for copy in small:
        copy.start()
    @pl.loop(0, slots)
    def _(s):
        k_copy(s).start()

    @pl.loop(0, slots)
    def _(s):
        v_copy(s).start()

    first_slot = lax.axis_index(SEQ) * slots
    first_lane = lax.axis_index(BLOCK) * slots
    lane = lax.broadcasted_iota(jnp.int32, (heads, page_len), 1)
    for copy in small:
        copy.wait()
    entry = table[...]
    code = (
        lax.broadcasted_iota(jnp.int32, entry.shape, 0) * max_pages
        + lax.broadcasted_iota(jnp.int32, entry.shape, 1)
        + 1
    ).astype(jnp.float32)
    owner_rows = out.shape[1] - (slots + PIECES) * share
    owner_row = jnp.zeros((owner_rows, page_len), jnp.float32)
    slot_queries = []
    valid_count = []
    for s in range(slots):
        found = jnp.max(jnp.where(entry == first_slot + s, code, 0.0)).astype(jnp.int32)
        index = jnp.maximum(found - 1, 0)
        request = index // max_pages
        page = index % max_pages
        row = batch_row[request]
        left = jnp.where(found > 0, lengths[request] - page * page_len, 0)
        valid_count.append(left)
        slot_queries.append(row)
        marked = jnp.where(found > 0, row + 1, 0).astype(jnp.float32)
        owner_row = jnp.where(lane[:owner_rows] == first_lane + s, marked, owner_row)

    scale = width ** (-0.5)
    level_rows = jnp.zeros((heads, page_len), jnp.float32)
    weights = []
    inverses = []
    for s in range(slots):
        if s % BATCH == 0:
            for n in range(s, s + BATCH):
                k_copy(n).wait()
        q = queries[slot_queries[s]]
        parts = []
        for k in range(heads_kv):
            full = lax.dot_general(
                q, k_buf[s, k], (((1,), (1,)), ((), ())), preferred_element_type=jnp.float32
            )
            parts.append(full[k * group : (k + 1) * group])
        valid = lane < valid_count[s]
        scores = jnp.where(valid, jnp.concatenate(parts, axis=0) * scale, NEG_BIG)
        top = jnp.max(scores, axis=1, keepdims=True)
        weight = jnp.where(valid, jnp.exp(scores - top), 0.0)
        total = jnp.sum(weight, axis=1, keepdims=True)
        live = total > 0.0
        total = jnp.where(live, total, 1.0)
        level = jnp.where(live, top + jnp.log(total), NEG_BIG)
        level_rows = jnp.where(lane == first_lane + s, level, level_rows)
        weights.append(weight.astype(jnp.bfloat16))
        inverses.append(1.0 / total)
    for s in range(slots):
        if s % BATCH == 0:
            for n in range(s, s + BATCH):
                v_copy(n).wait()
        for k in range(heads_kv):
            full = jnp.dot(weights[s], v_buf[s, k], preferred_element_type=jnp.float32)
            lines = slice(k * group, (k + 1) * group)
            rows[s * heads + k * group : s * heads + (k + 1) * group] = (
                full[lines] * inverses[s][lines]
            )
    for n, piece in enumerate(pieces_of(level_rows)):
        stats[n * heads : (n + 1) * heads] = piece
    for p in range(peers):
        for h in range(share):
            line = rows[pl.ds(p * share + h, slots, stride=heads)]
            out[p, h * slots : (h + 1) * slots] = line.astype(jnp.bfloat16)
        first = p * share
        lines = [stats[n * heads + first : n * heads + first + share] for n in range(PIECES)]
        out[p, share * slots :] = jnp.concatenate(lines + [owner_row], axis=0).astype(jnp.bfloat16)


def pieces_of(x):
    high = x.astype(jnp.bfloat16).astype(jnp.float32)
    rest = x - high
    middle = rest.astype(jnp.bfloat16).astype(jnp.float32)
    return high, middle, (rest - middle).astype(jnp.bfloat16).astype(jnp.float32)


def merge_slots_kernel(share, slots, got, out):
    peers, height, width = got.shape
    count = peers * slots
    requests = (out.shape[0] - STAT_ROWS) // share
    stat = got[0, share * slots :].astype(jnp.float32)
    for i in range(1, peers):
        stat = stat + got[i, share * slots :].astype(jnp.float32)
    owner = stat[PIECES * share : PIECES * share + 1].astype(jnp.int32) - 1
    owned = owner == lax.broadcasted_iota(jnp.int32, (requests, width), 0)
    levels = []
    for h in range(share):
        data = got[:, h * slots : (h + 1) * slots].astype(jnp.float32).reshape(count, width)
        level = stat[h : h + 1] + stat[share + h : share + h + 1]
        level = level + stat[2 * share + h : 2 * share + h + 1]
        top = jnp.max(jnp.where(owned, level, NEG_BIG), axis=1, keepdims=True)
        factor = jnp.where(owned, jnp.exp(level - top), 0.0)
        total = jnp.sum(factor, axis=1, keepdims=True)
        merged = jnp.dot(
            factor[:, :count], data, precision=lax.Precision.HIGHEST, preferred_element_type=jnp.float32
        )
        live = total > 0.0
        total = jnp.where(live, total, 1.0)
        out[h * requests : (h + 1) * requests] = (merged / total).astype(jnp.bfloat16)
        levels.append(jnp.where(live, top + jnp.log(total), NEG_BIG))
    lane = lax.broadcasted_iota(jnp.int32, (share * requests, width), 1)
    table = jnp.zeros((share * requests, width), jnp.float32)
    for n, piece in enumerate(pieces_of(jnp.concatenate(levels, axis=0))):
        table = jnp.where(lane == n, piece, table)
    out[share * requests :] = jnp.transpose(table)[:STAT_ROWS].astype(jnp.bfloat16)


def merge_blocks_kernel(*refs):
    *got, out = refs
    blocks = len(got)
    height, width = got[0].shape
    count = height - STAT_ROWS
    levels = []
    for j in range(blocks):
        tile = got[j][count:].astype(jnp.float32)
        levels.append(tile[0:1] + tile[1:2] + tile[2:3])
    level = jnp.concatenate(levels, axis=0)
    share = jnp.exp(level - jnp.max(level, axis=0, keepdims=True))
    share = share / jnp.sum(share, axis=0, keepdims=True)
    square = jnp.concatenate([share, jnp.zeros((width - blocks, width), jnp.float32)], axis=0)
    column = jnp.transpose(square)[:count]
    result = column[:, 0:1] * got[0][:count].astype(jnp.float32)
    for j in range(1, blocks):
        result = result + column[:, j : j + 1] * got[j][:count].astype(jnp.float32)
    out[...] = result.astype(jnp.bfloat16)


def pick_kernel(holders, *refs):
    *sent, out = refs
    block = lax.axis_index("far")
    for members, ref in zip(holders, sent):
        here = functools.reduce(jnp.logical_or, [block == j for j in members])

        @pl.when(here)
        def _(ref=ref):
            row = ref[...]
            if len(out.shape) == len(ref.shape):
                out[...] = row
            else:
                for p in range(out.shape[0]):
                    out[p] = row


def in_vmem():
    return pl.BlockSpec(memory_space=pltpu.VMEM)


def kept(shape, dtype):
    return pltpu.VMEM(shape, dtype)


def near(x):
    return pltpu.with_memory_space_constraint(x, pltpu.VMEM)


def shards(blocks, queries, k_cache, value_cache, kv_lengths, page_table, request_batch_row):
    slots, heads_kv, page_len, width = k_cache.shape
    requests, heads, _ = queries.shape
    peers = NEAR * ACROSS
    lines = -(-((slots + PIECES) * (heads // peers) + 1) // 8) * 8
    share = heads // peers
    partial = pl.pallas_call(
        attend_kernel,
        out_shape=kept((peers, lines, width), jnp.bfloat16),
        in_specs=[pl.BlockSpec(memory_space=pl.ANY)] * 6,
        out_specs=in_vmem(),
        scratch_shapes=[
            pltpu.SMEM(request_batch_row.shape, jnp.int32),
            pltpu.SMEM(kv_lengths.shape, jnp.int32),
            pltpu.VMEM(page_table.shape, jnp.int32),
            pltpu.VMEM(queries.shape, queries.dtype),
            pltpu.VMEM(k_cache.shape, k_cache.dtype),
            pltpu.VMEM(value_cache.shape, value_cache.dtype),
            pltpu.VMEM((slots * heads, width), jnp.float32),
            pltpu.VMEM((PIECES * heads, page_len), jnp.float32),
            pltpu.SemaphoreType.DMA((2, slots)),
            pltpu.SemaphoreType.DMA((4,)),
        ],
        name="attend",
    )(request_batch_row, kv_lengths, page_table, queries, k_cache, value_cache)
    partial = lax.all_to_all(partial, BLOCK, 0, 0)
    merged = pl.pallas_call(
        functools.partial(merge_slots_kernel, share, slots),
        out_shape=kept((share * requests + STAT_ROWS, width), jnp.bfloat16),
        in_specs=[in_vmem()],
        out_specs=in_vmem(),
        name="merge_slots",
    )(near(partial))
    def send(x, pairs):
        return lax.ppermute(x, "far", pairs)

    half = ROOT + blocks // 2
    late = sorted(range(half, blocks), key=lambda j: abs(2 * j - half - blocks))
    sources = [*late, ROOT - 1, *range(half - 1, ROOT, -1)]
    pieces = [merged] + [send(merged, [(j, ROOT)]) for j in reversed(sources)]
    result = pl.pallas_call(
        merge_blocks_kernel,
        out_shape=kept((share * requests, width), jnp.bfloat16),
        in_specs=[in_vmem()] * blocks,
        out_specs=in_vmem(),
        name="merge_blocks",
    )(*[near(piece) for piece in pieces])
    def pick(holders, arrays, shape):
        return pl.pallas_call(
            functools.partial(pick_kernel, holders),
            out_shape=kept(shape, jnp.bfloat16),
            in_specs=[in_vmem()] * len(arrays),
            out_specs=in_vmem(),
            name="pick",
        )(*[near(array) for array in arrays])

    shape = (share * requests, width)
    holders = [(ROOT,)] + [(j,) for j in reversed(FIRST)]
    sent = [result] + [send(result, [(ROOT, j)]) for j in reversed(FIRST)]
    for pairs in TURNS:
        result = pick(holders, sent, shape)
        sent = [result, send(result, list(pairs))]
        holders = [tuple(j for held in holders for j in held), tuple(j for _, j in pairs)]
    finished = pick(holders, sent, (peers, *shape))
    finished = lax.all_to_all(finished, BLOCK, 0, 0)
    return finished.reshape(heads, requests, width).transpose(1, 0, 2)


def solution(mesh):
    blocks = mesh.shape["seq"] // (NEAR * ACROSS)
    finer = Mesh(
        mesh.devices.reshape(mesh.shape["group"], blocks, NEAR, ACROSS, mesh.shape["tensor"]),
        ("group", "far", "near", "across", "tensor"),
    )
    placed = (
        P("group", "tensor", None),
        P(GROUP_SEQ, "tensor", None, None),
        P(GROUP_SEQ, "tensor", None, None),
        P("group"),
        P("group", None),
        P("group"),
    )
    return jax.shard_map(
        functools.partial(shards, blocks),
        mesh=finer,
        in_specs=placed,
        out_specs=P("group", "tensor", None),
        check_vma=False,
    )
```

```python
import functools

import jax
import jax.numpy as jnp
from jax import lax
from jax.experimental import pallas as pl
from jax.experimental.pallas import tpu as pltpu
from jax.sharding import Mesh
from jax.sharding import PartitionSpec as P

NEG_BIG = -1e30
ACROSS = 4
NEAR = 2
BLOCK = ("near", "across")
SEQ = ("far", "near", "across")
GROUP_SEQ = ("group", "far", "near", "across")
PIECES = 3
STAT_ROWS = 8
FIRST = (0, 2, 10, 6, 13)
TURNS = (
    ((2, 3), (10, 12), (13, 14), (6, 8)),
    ((3, 4), (6, 5), (8, 7), (10, 9), (12, 11), (14, 15)),
)
BATCH = 8
ROOT = 1


def attend_kernel(
    batch_row_hbm,
    lengths_hbm,
    table_hbm,
    queries_hbm,
    k_hbm,
    v_hbm,
    out,
    batch_row,
    lengths,
    table,
    queries,
    k_buf,
    v_buf,
    rows,
    stats,
    sems,
    small_sems,
):
    slots, heads_kv, page_len, width = k_buf.shape
    heads = queries.shape[1]
    group = heads // heads_kv
    peers = out.shape[0]
    share = heads // peers
    max_pages = table.shape[1]

    def k_copy(s):
        return pltpu.make_async_copy(k_hbm.at[s], k_buf.at[s], sems.at[0, s])

    def v_copy(s):
        return pltpu.make_async_copy(v_hbm.at[s], v_buf.at[s], sems.at[1, s])

    small = [
        pltpu.make_async_copy(source, target, small_sems.at[n])
        for n, (source, target) in enumerate(
            [
                (table_hbm, table),
                (batch_row_hbm, batch_row),
                (lengths_hbm, lengths),
                (queries_hbm, queries),
            ]
        )
    ]
    for copy in small:
        copy.start()
    @pl.loop(0, slots)
    def _(s):
        k_copy(s).start()

    @pl.loop(0, slots)
    def _(s):
        v_copy(s).start()

    first_slot = lax.axis_index(SEQ) * slots
    first_lane = lax.axis_index(BLOCK) * slots
    lane = lax.broadcasted_iota(jnp.int32, (heads, page_len), 1)
    for copy in small:
        copy.wait()
    entry = table[...]
    code = (
        lax.broadcasted_iota(jnp.int32, entry.shape, 0) * max_pages
        + lax.broadcasted_iota(jnp.int32, entry.shape, 1)
        + 1
    ).astype(jnp.float32)
    owner_rows = out.shape[1] - (slots + PIECES) * share
    owner_row = jnp.zeros((owner_rows, page_len), jnp.float32)
    slot_queries = []
    valid_count = []
    for s in range(slots):
        found = jnp.max(jnp.where(entry == first_slot + s, code, 0.0)).astype(jnp.int32)
        index = jnp.maximum(found - 1, 0)
        request = index // max_pages
        page = index % max_pages
        row = batch_row[request]
        left = jnp.where(found > 0, lengths[request] - page * page_len, 0)
        valid_count.append(left)
        slot_queries.append(row)
        marked = jnp.where(found > 0, row + 1, 0).astype(jnp.float32)
        owner_row = jnp.where(lane[:owner_rows] == first_lane + s, marked, owner_row)

    scale = width ** (-0.5)
    level_rows = jnp.zeros((heads, page_len), jnp.float32)
    weights = []
    inverses = []
    for s in range(slots):
        if s % BATCH == 0:
            for n in range(s, s + BATCH):
                k_copy(n).wait()
        q = queries[slot_queries[s]]
        parts = []
        for k in range(heads_kv):
            full = lax.dot_general(
                q, k_buf[s, k], (((1,), (1,)), ((), ())), preferred_element_type=jnp.float32
            )
            parts.append(full[k * group : (k + 1) * group])
        valid = lane < valid_count[s]
        scores = jnp.where(valid, jnp.concatenate(parts, axis=0) * scale, NEG_BIG)
        top = jnp.max(scores, axis=1, keepdims=True)
        weight = jnp.where(valid, jnp.exp(scores - top), 0.0)
        total = jnp.sum(weight, axis=1, keepdims=True)
        live = total > 0.0
        total = jnp.where(live, total, 1.0)
        level = jnp.where(live, top + jnp.log(total), NEG_BIG)
        level_rows = jnp.where(lane == first_lane + s, level, level_rows)
        weights.append(weight.astype(jnp.bfloat16))
        inverses.append(1.0 / total)
    for s in range(slots):
        if s % BATCH == 0:
            for n in range(s, s + BATCH):
                v_copy(n).wait()
        for k in range(heads_kv):
            full = jnp.dot(weights[s], v_buf[s, k], preferred_element_type=jnp.float32)
            lines = slice(k * group, (k + 1) * group)
            rows[s * heads + k * group : s * heads + (k + 1) * group] = (
                full[lines] * inverses[s][lines]
            )
    for n, piece in enumerate(pieces_of(level_rows)):
        stats[n * heads : (n + 1) * heads] = piece
    for p in range(peers):
        for h in range(share):
            line = rows[pl.ds(p * share + h, slots, stride=heads)]
            out[p, h * slots : (h + 1) * slots] = line.astype(jnp.bfloat16)
        first = p * share
        lines = [stats[n * heads + first : n * heads + first + share] for n in range(PIECES)]
        out[p, share * slots :] = jnp.concatenate(lines + [owner_row], axis=0).astype(jnp.bfloat16)


def pieces_of(x):
    high = x.astype(jnp.bfloat16).astype(jnp.float32)
    rest = x - high
    middle = rest.astype(jnp.bfloat16).astype(jnp.float32)
    return high, middle, (rest - middle).astype(jnp.bfloat16).astype(jnp.float32)


def merge_slots_kernel(share, slots, got, out):
    peers, height, width = got.shape
    count = peers * slots
    requests = (out.shape[0] - STAT_ROWS) // share
    stat = got[0, share * slots :].astype(jnp.float32)
    for i in range(1, peers):
        stat = stat + got[i, share * slots :].astype(jnp.float32)
    owner = stat[PIECES * share : PIECES * share + 1].astype(jnp.int32) - 1
    owned = owner == lax.broadcasted_iota(jnp.int32, (requests, width), 0)
    levels = []
    for h in range(share):
        data = got[:, h * slots : (h + 1) * slots].astype(jnp.float32).reshape(count, width)
        level = stat[h : h + 1] + stat[share + h : share + h + 1]
        level = level + stat[2 * share + h : 2 * share + h + 1]
        top = jnp.max(jnp.where(owned, level, NEG_BIG), axis=1, keepdims=True)
        factor = jnp.where(owned, jnp.exp(level - top), 0.0)
        total = jnp.sum(factor, axis=1, keepdims=True)
        merged = jnp.dot(
            factor[:, :count], data, precision=lax.Precision.HIGHEST, preferred_element_type=jnp.float32
        )
        live = total > 0.0
        total = jnp.where(live, total, 1.0)
        out[h * requests : (h + 1) * requests] = (merged / total).astype(jnp.bfloat16)
        levels.append(jnp.where(live, top + jnp.log(total), NEG_BIG))
    lane = lax.broadcasted_iota(jnp.int32, (share * requests, width), 1)
    table = jnp.zeros((share * requests, width), jnp.float32)
    for n, piece in enumerate(pieces_of(jnp.concatenate(levels, axis=0))):
        table = jnp.where(lane == n, piece, table)
    out[share * requests :] = jnp.transpose(table)[:STAT_ROWS].astype(jnp.bfloat16)


def merge_blocks_kernel(*refs):
    *got, out = refs
    blocks = len(got)
    height, width = got[0].shape
    count = height - STAT_ROWS
    levels = []
    for j in range(blocks):
        tile = got[j][count:].astype(jnp.float32)
        levels.append(tile[0:1] + tile[1:2] + tile[2:3])
    level = jnp.concatenate(levels, axis=0)
    share = jnp.exp(level - jnp.max(level, axis=0, keepdims=True))
    share = share / jnp.sum(share, axis=0, keepdims=True)
    square = jnp.concatenate([share, jnp.zeros((width - blocks, width), jnp.float32)], axis=0)
    column = jnp.transpose(square)[:count]
    result = column[:, 0:1] * got[0][:count].astype(jnp.float32)
    for j in range(1, blocks):
        result = result + column[:, j : j + 1] * got[j][:count].astype(jnp.float32)
    out[...] = result.astype(jnp.bfloat16)


def pick_kernel(holders, *refs):
    *sent, out = refs
    block = lax.axis_index("far")
    for members, ref in zip(holders, sent):
        here = functools.reduce(jnp.logical_or, [block == j for j in members])

        @pl.when(here)
        def _(ref=ref):
            row = ref[...]
            if len(out.shape) == len(ref.shape):
                out[...] = row
            else:
                for p in range(out.shape[0]):
                    out[p] = row


def in_vmem():
    return pl.BlockSpec(memory_space=pltpu.VMEM)


def kept(shape, dtype):
    return pltpu.VMEM(shape, dtype)


def near(x):
    return pltpu.with_memory_space_constraint(x, pltpu.VMEM)


def shards(blocks, queries, k_cache, value_cache, kv_lengths, page_table, request_batch_row):
    slots, heads_kv, page_len, width = k_cache.shape
    requests, heads, _ = queries.shape
    peers = NEAR * ACROSS
    lines = -(-((slots + PIECES) * (heads // peers) + 1) // 8) * 8
    share = heads // peers
    partial = pl.pallas_call(
        attend_kernel,
        out_shape=kept((peers, lines, width), jnp.bfloat16),
        in_specs=[pl.BlockSpec(memory_space=pl.ANY)] * 6,
        out_specs=in_vmem(),
        scratch_shapes=[
            pltpu.SMEM(request_batch_row.shape, jnp.int32),
            pltpu.SMEM(kv_lengths.shape, jnp.int32),
            pltpu.VMEM(page_table.shape, jnp.int32),
            pltpu.VMEM(queries.shape, queries.dtype),
            pltpu.VMEM(k_cache.shape, k_cache.dtype),
            pltpu.VMEM(value_cache.shape, value_cache.dtype),
            pltpu.VMEM((slots * heads, width), jnp.float32),
            pltpu.VMEM((PIECES * heads, page_len), jnp.float32),
            pltpu.SemaphoreType.DMA((2, slots)),
            pltpu.SemaphoreType.DMA((4,)),
        ],
        name="attend",
    )(request_batch_row, kv_lengths, page_table, queries, k_cache, value_cache)
    partial = lax.all_to_all(partial, BLOCK, 0, 0)
    merged = pl.pallas_call(
        functools.partial(merge_slots_kernel, share, slots),
        out_shape=kept((share * requests + STAT_ROWS, width), jnp.bfloat16),
        in_specs=[in_vmem()],
        out_specs=in_vmem(),
        name="merge_slots",
    )(near(partial))
    def send(x, pairs):
        return lax.ppermute(x, "far", pairs)

    half = ROOT + blocks // 2
    late = sorted(range(half, blocks), key=lambda j: abs(2 * j - half - blocks))
    sources = [*late, ROOT - 1, *range(half - 1, ROOT, -1)]
    pieces = [merged] + [send(merged, [(j, ROOT)]) for j in reversed(sources)]
    result = pl.pallas_call(
        merge_blocks_kernel,
        out_shape=kept((share * requests, width), jnp.bfloat16),
        in_specs=[in_vmem()] * blocks,
        out_specs=in_vmem(),
        name="merge_blocks",
    )(*[near(piece) for piece in pieces])
    def pick(holders, arrays, shape):
        return pl.pallas_call(
            functools.partial(pick_kernel, holders),
            out_shape=kept(shape, jnp.bfloat16),
            in_specs=[in_vmem()] * len(arrays),
            out_specs=in_vmem(),
            name="pick",
        )(*[near(array) for array in arrays])

    shape = (share * requests, width)
    holders = [(ROOT,)] + [(j,) for j in reversed(FIRST)]
    sent = [result] + [send(result, [(ROOT, j)]) for j in reversed(FIRST)]
    for pairs in TURNS:
        result = pick(holders, sent, shape)
        sent = [result, send(result, list(pairs))]
        holders = [tuple(j for held in holders for j in held), tuple(j for _, j in pairs)]
    finished = pick(holders, sent, (peers, *shape))
    finished = lax.all_to_all(finished, BLOCK, 0, 0)
    return finished.reshape(heads, requests, width).transpose(1, 0, 2)


def solution(mesh):
    blocks = mesh.shape["seq"] // (NEAR * ACROSS)
    finer = Mesh(
        mesh.devices.reshape(mesh.shape["group"], blocks, NEAR, ACROSS, mesh.shape["tensor"]),
        ("group", "far", "near", "across", "tensor"),
    )
    placed = (
        P("group", "tensor", None),
        P(GROUP_SEQ, "tensor", None, None),
        P(GROUP_SEQ, "tensor", None, None),
        P("group"),
        P("group", None),
        P("group"),
    )
    return jax.shard_map(
        functools.partial(shards, blocks),
        mesh=finer,
        in_specs=placed,
        out_specs=P("group", "tensor", None),
        check_vma=False,
    )
```
